512 devices in a mesh: mem: 128 (over x, y, z_lo), slab: 4 (over z_hi, core).
Axes of the slice: x: 4, y: 4, z: 16 (z_hi: 2, z_lo: 8; z = z_hi * 8 + z_lo), core: 2. Of those that a mesh axis runs over, the one named last changes fastest.
Arguments:
- prior_sample_stack: float32 [128, 3, 256, 512], P('mem', None, None, 'slab'), may hold values from -4 to 4
- obs_cell: int32 [128, 512], P('mem', 'slab'), may hold values from 0 to 255
- obs_value: float32 [128, 512], P('mem', 'slab'), may hold values from -4 to 4
- obs_bin: int32 [128, 512], P('mem', 'slab'), may hold values from 0 to 3
Outputs:
- analysis: float32 [128, 3, 256, 512], P('mem', None, None, 'slab')
The draws below stay inside these ranges and needn't reach their ends.
Inputs may be any that keep to these rules, and one draw needn't show every extreme that they name: obs_cell is local row times 128 plus local column within the observation's region rows and its index of slab's columns.
All inputs are finite; a program needn't handle non-finite values.
Results may differ from the reference program's by a relative error of at most 0.0003.
Values sent between devices are 32-bit elements; how exact they have to be, the bound alone decides.
A program may use at most 64 MiB of HBM per device.

```python
import math
import jax
import jax.numpy as jnp
from jax import lax

LATITUDE_COUNT = 2
CY = 128
OBS_REG = 128
STEPS = 12
SWEEPS = 8
MEMBERS = 128
REGIONS = 128
NX = 256
NY = 512
N_SLAB = 4


def with_ends(array, key, low, high):
    place = [jax.random.randint(jax.random.fold_in(key, axis), (), 0, length) for axis, length in enumerate(array.shape)]
    longest = array.shape.index(max(array.shape))
    beside = place[:longest] + [(place[longest] + 1) % array.shape[longest]] + place[longest + 1:]
    return array.at[tuple(place)].set(low).at[tuple(beside)].set(high)


def level_of(rng, extent, shards, least, largest):
    level = 1.0
    for axis_at, blocks in shards:
        heights = jax.random.uniform(jax.random.fold_in(jax.random.fold_in(rng, 6), axis_at), (blocks,), jnp.float32, least / len(shards), largest / len(shards))
        level = level * jnp.repeat(jnp.exp(heights), extent[axis_at] // blocks).reshape((-1,) + (1,) * (len(extent) - 1 - axis_at))
    return level


def noise(stream_key, dims, scale, limit, cuts=(), kind=jnp.bfloat16):
    result = jax.random.normal(stream_key, dims, jnp.float32) * scale
    if len(cuts) > 0:
        result = level_of(stream_key, dims, cuts, -0.22, 0.18) * result
    return jnp.clip(result, min=-limit, max=limit).astype(kind)


def setup_inputs(seed: int = 0) -> dict:
    arg_keys = jax.random.split(jax.random.key(seed), 5)
    return {
        "prior_sample_stack": noise(arg_keys[0], (MEMBERS, 3, NX, NY), 0.3, 4.0, ((0, 128), (3, 4)), jnp.float32),
        "obs_cell": with_ends(jax.random.randint(arg_keys[1], (REGIONS, N_SLAB * OBS_REG), 0, LATITUDE_COUNT * CY), jax.random.fold_in(arg_keys[1], 1), 0, (LATITUDE_COUNT * CY) - 1).astype(jnp.int32),
        "obs_value": noise(arg_keys[2], (REGIONS, N_SLAB * OBS_REG), 0.5, 4.0, ((0, 128), (1, 4)), jnp.float32),
        "obs_bin": with_ends(jax.random.randint(arg_keys[3], (REGIONS, N_SLAB * OBS_REG), 0, 4), jax.random.fold_in(arg_keys[3], 1), 0, 3).astype(jnp.int32),
    }


time_step = 0.25
gravity = 1.0
mean_depth = 1.0
coriolis = 0.2
viscosity = 0.4
inflation = 1.1
highest = lax.Precision.HIGHEST

def centre(values):
    return values[:, 1:-1]

def east_of(values):
    return jnp.roll(values[:, 1:-1], -1, 0)

def west_of(values):
    return jnp.roll(values[:, 1:-1], 1, 0)

def north_of(values):
    return values[:, 2:]

def south_of(values):
    return values[:, :-2]

def spread(values):
    return east_of(values) + west_of(values) + north_of(values) + south_of(values) - 4.0 * centre(values)

def slope_x(values):
    return 0.5 * (east_of(values) - west_of(values))

def slope_y(values):
    return 0.5 * (north_of(values) - south_of(values))

def advance(padded):
    elevation_anomaly = padded[0]
    east_wind = padded[1]
    north_wind = padded[2]
    flux_x = (mean_depth + elevation_anomaly) * east_wind
    flux_y = (mean_depth + elevation_anomaly) * north_wind
    east_mid = centre(east_wind)
    north_mid = centre(north_wind)
    new_height = centre(elevation_anomaly) + time_step * (viscosity * spread(elevation_anomaly) - slope_x(flux_x) - slope_y(flux_y))
    new_east = east_mid + time_step * (viscosity * spread(east_wind) - east_mid * slope_x(east_wind) - north_mid * slope_y(east_wind) - gravity * slope_x(elevation_anomaly) + coriolis * north_mid)
    new_north = north_mid + time_step * (viscosity * spread(north_wind) - east_mid * slope_x(north_wind) - north_mid * slope_y(north_wind) - gravity * slope_y(elevation_anomaly) - coriolis * east_mid)
    return jnp.stack([new_height, new_east, new_north])

def partial_sums(anomaly, distance, obs_weight, innovation, band_rows):
    target = jnp.arange(band_rows).astype(jnp.float32)
    scaled_dist = (distance[None, :] - target[:, None]) / float(band_rows)
    weight = obs_weight[None, :] * jnp.exp(-0.5 * scaled_dist * scaled_dist)
    scaled = anomaly[None, :, :] * weight[:, None, :]
    gram_matrix = jnp.einsum('tmj,kj->tmk', scaled, anomaly, precision=highest)
    pull_vector = jnp.einsum('tmj,j->tm', scaled, innovation, precision=highest)
    return (gram_matrix, pull_vector)

def batch_product(left, right):
    return jnp.einsum('tij,tjk->tik', left, right, precision=highest)

def weights_from(gram_matrix, pull_vector, members):
    identity = jnp.eye(members, dtype=jnp.float32)
    gram_matrix = gram_matrix + (members - 1) / inflation * identity[None]
    traces = jnp.trace(gram_matrix, axis1=1, axis2=2)
    iterate = gram_matrix / traces[:, None, None]
    inverse = jnp.broadcast_to(identity, gram_matrix.shape)
    for iteration in range(SWEEPS):
        correction = 1.5 * identity[None] - 0.5 * batch_product(inverse, iterate)
        iterate, inverse = (batch_product(iterate, correction), batch_product(correction, inverse))
    inv_root = inverse / jnp.sqrt(traces)[:, None, None]
    inner = jnp.einsum('tij,tj->ti', inv_root, pull_vector, precision=highest)
    mean_weights = jnp.einsum('tij,tj->ti', inv_root, inner, precision=highest)
    return math.sqrt(members - 1) * inv_root + mean_weights[:, :, None]

def apply_weights(zone_portion, mixing):
    mean_state = lax.optimization_barrier(jnp.mean(zone_portion, axis=0))
    spread_state = zone_portion - mean_state[None]
    return mean_state[None] + jnp.einsum('mftc,tmk->kftc', spread_state, mixing, precision=highest)

def realization_prediction(sample_realization):

    def one_step(counter, values):
        padded = jnp.concatenate([values[:, :, -1:], values, values[:, :, :1]], axis=2)
        return advance(padded)
    return lax.fori_loop(0, STEPS, one_step, sample_realization)

def reference(prior_sample_stack, obs_cell, obs_value, obs_bin):
    predicted_grid = lax.map(realization_prediction, prior_sample_stack)
    elevation_anomaly = predicted_grid[:, 0]
    slab_of = (jnp.arange(N_SLAB * OBS_REG) // OBS_REG).astype(jnp.int32)
    region_ids = jnp.arange(REGIONS).astype(jnp.int32)
    obs_rows = region_ids[:, None] * LATITUDE_COUNT + obs_cell // CY
    obs_columns = slab_of[None, :] * CY + obs_cell % CY
    observed = elevation_anomaly[:, obs_rows, obs_columns]
    obs_mean = lax.optimization_barrier(jnp.mean(observed, axis=0))
    anomaly_all = jnp.transpose(observed - obs_mean[None], (1, 0, 2))
    innovation_all = obs_value - obs_mean
    weight_all = 10.0 / (1.0 + obs_bin.astype(jnp.float32))
    local_rows = (obs_cell // CY).astype(jnp.float32)
    offsets = jnp.arange(-2, 3).astype(jnp.int32)

    def analyse(zone_portion_range):
        chosen = (zone_portion_range + offsets) % REGIONS
        anomaly = jnp.moveaxis(anomaly_all[chosen], 0, 1).reshape(MEMBERS, -1)
        distance = ((offsets * LATITUDE_COUNT).astype(jnp.float32)[:, None] + local_rows[chosen]).reshape(-1)
        gram_matrix, pull_vector = partial_sums(anomaly, distance, weight_all[chosen].reshape(-1), innovation_all[chosen].reshape(-1), LATITUDE_COUNT)
        mixing = weights_from(gram_matrix, pull_vector, MEMBERS)
        zone_portion = lax.dynamic_slice_in_dim(predicted_grid, (zone_portion_range * LATITUDE_COUNT).astype(jnp.int32), LATITUDE_COUNT, 2)
        return apply_weights(zone_portion, mixing)
    analysed = lax.map(analyse, region_ids)
    return jnp.transpose(analysed, (1, 2, 0, 3, 4)).reshape(MEMBERS, 3, NX, NY)
```

```python
import math

import jax
import jax.numpy as jnp
from jax import lax
from jax.experimental import pallas as pl
from jax.experimental.pallas import tpu as pltpu
from jax.sharding import PartitionSpec as P

STEPS = 12
SWEEPS = 8
SIZE = 32
BATCH = (16, 16, 16)
MESH = pl.DeviceIdType.MESH
F32 = jnp.float32
BF16 = jnp.bfloat16

BASE = 24
ROWS = BASE + 128 + BASE
OFFSETS = (1, -1, 2, -2)
ORDER = (0, 7, 1, 6, 2, 5, 3, 4)


def device_of(x, y, z, core):
    return ((x * 4 + y) * 8 + z % 8, (z // 8) * 2 + core)


def region_at(x, y, k):
    pos = y * 4 + x + (y % 2) * (3 - 2 * x)
    pos = pos + (k % 2) * (15 - 2 * pos)
    return k * 16 + pos


def place_of(region):
    k, pos = region // 16, region % 16
    pos = pos + (k % 2) * (15 - 2 * pos)
    y, x = pos // 4, pos % 4
    return x + (y % 2) * (3 - 2 * x), y, k


def halves(a):
    hi = a.astype(BF16)
    return hi, (a - hi.astype(F32)).astype(BF16)


def as_lhs(a):
    return jnp.concatenate(halves(a), axis=1)


def as_rhs(b):
    row = jnp.concatenate(halves(b), axis=1)
    return jnp.concatenate([row, row], axis=0)


def product(lhs, rhs):
    r = jnp.dot(lhs, rhs, preferred_element_type=F32)
    return r[:, :128] + r[:, 128:]


def forecast_block(src, dst, row, size):
    c, n, s = {}, {}, {}
    for f in range(3):
        for t in range(2):
            c[f, t] = src[f, t, row : row + size]
            n[f, t] = src[f, t, row + 1 : row + 1 + size]
            s[f, t] = src[f, t, row - 1 : row - 1 + size]
    for t in range(2):
        if t == 0:
            e = [c[f, 1] for f in range(3)]
            w = [pltpu.roll(c[f, 1], 1, 1) for f in range(3)]
        else:
            e = [pltpu.roll(c[f, 0], 127, 1) for f in range(3)]
            w = [c[f, 0] for f in range(3)]
        h, u, v = (c[f, t] for f in range(3))
        hn, un, vn = (n[f, t] for f in range(3))
        hs, us, vs = (s[f, t] for f in range(3))
        he, ue, ve = e
        hw, uw, vw = w
        flux = (1.0 + he) * ue - (1.0 + hw) * uw + (1.0 + hn) * vn - (1.0 + hs) * vs
        a, b = 0.125 * u, 0.125 * v
        dst[0, t, row : row + size] = 0.6 * h + 0.1 * (he + hw + hn + hs) - 0.125 * flux
        dst[1, t, row : row + size] = (
            0.6 * u + 0.1 * (ue + uw + un + us) - (a * (ue - uw) + b * (un - us)) - 0.125 * (he - hw) + 0.05 * v
        )
        dst[2, t, row : row + size] = (
            0.6 * v + 0.1 * (ve + vw + vn + vs) - (a * (ve - vw) + b * (vn - vs)) - 0.125 * (hn - hs) - 0.05 * u
        )


def kernel(
    prior, cell, value, bins, out,
    nat, state, halo_out, halo_in, obs_out, obs_in, heights_out, winds_out, heights, winds,
    parts, parts_in, chunk, chunk_in, grams, back_out, back,
    load_sem, halo_send, halo_recv, obs_send, obs_recv, a2a_send, a2a_recv,
    part_send, part_recv, chunk_send, chunk_recv, gram_send, gram_recv, lines,
):
    m, slab = lax.axis_index("mem"), lax.axis_index("slab")
    x, y, zl = m // 32, (m // 8) % 4, m % 8
    z_hi, core = slab // 2, slab % 2
    z = z_hi * 8 + zl
    k, par = z // 2, z % 2
    region = region_at(x, y, k)
    ident = par * 2 + core
    away = (z_hi + par) % 2

    def remote(src, dst, send, recv, where):
        return pltpu.make_async_remote_copy(
            src_ref=src, dst_ref=dst, send_sem=send, recv_sem=recv, device_id=where, device_id_type=MESH
        )

    def group(i):
        return device_of(x, y, 2 * k + i // 2, i % 2)

    def neighbour(o):
        nx, ny, nk = place_of((region + o + 128) % 128)
        return device_of(nx, ny, 2 * nk + par, core)

    load = pltpu.make_async_copy(prior, nat, load_sem)
    load.start()

    barrier = pltpu.get_barrier_semaphore()

    def greet(where):
        pl.semaphore_signal(barrier, inc=1, device_id=where, device_id_type=MESH)

    for side in (1, 3):
        greet((m, (slab + side) % 4))
    for j in range(1, 4):
        greet(group((ident + j) % 4))
    for o in OFFSETS:
        greet(neighbour(o))

    def in_plane(j):
        return ((x + j % 4) % 4 * 4 + (y + j // 4) % 4) * 8 + zl, slab

    def greet_line_and_plane(j, carry):
        pz = (z + j) % 16
        greet((m - zl + pz % 8, (pz // 8) * 2 + core))
        greet(in_plane(j))
        return carry

    def tell_plane(j, carry):
        pl.semaphore_signal(lines, inc=1, device_id=in_plane(j), device_id_type=MESH)
        return carry

    lax.fori_loop(1, 16, greet_line_and_plane, 0)
    load.wait()
    for f in range(3):
        for t in range(2):
            state[0, f, t, BASE : BASE + 128] = nat[f, pl.ds(t, 128, stride=2), :].T
            i = (f * 2 + t) * 12
            halo_out[0, i : i + 12] = state[0, f, t, BASE : BASE + 12]
            halo_out[1, i : i + 12] = state[0, f, t, BASE + 116 : BASE + 128]
    halo = [
        remote(halo_out.at[0], halo_in.at[0], halo_send.at[0], halo_recv.at[0], (m, (slab + 3) % 4)),
        remote(halo_out.at[1], halo_in.at[1], halo_send.at[1], halo_recv.at[1], (m, (slab + 1) % 4)),
    ]

    pl.semaphore_wait(barrier, 39)
    for copy in halo:
        copy.start()
    lax.fori_loop(1, 16, tell_plane, 0)

    for copy in halo:
        copy.wait()
    for f in range(3):
        for t in range(2):
            i = (f * 2 + t) * 12
            state[0, f, t, BASE + 128 : BASE + 140] = halo_in[0, i : i + 12]
            state[0, f, t, BASE - 12 : BASE] = halo_in[1, i : i + 12]

    def two_steps(counter, carry):
        for now in range(2):
            for block in range(160 // SIZE):
                forecast_block(state.at[now], state.at[1 - now], BASE - 16 + SIZE * block, SIZE)
        return carry

    lax.fori_loop(0, STEPS // 2, two_steps, 0)

    pl.semaphore_wait(lines, 15)

    ox, oy, ok = place_of(m)
    obs_out[0:1] = cell[...].astype(F32)
    obs_out[1:2] = value[...]
    obs_out[2:3] = bins[...].astype(F32)
    obs_where = device_of(ox, oy, 2 * ok + z_hi, core)
    obs_copy = remote(obs_out, obs_in, obs_send, obs_recv, obs_where)
    obs_home = jnp.logical_and(obs_where[0] == m, obs_where[1] == slab)

    @pl.when(jnp.logical_not(obs_home))
    def _():
        obs_copy.start()

    @pl.when(obs_home)
    def _():
        obs_in[...] = obs_out[...]

    for t in range(2):
        heights_out[:, t, :] = state[0, 0, t, BASE : BASE + 128].T
    for f in range(1, 3):
        for t in range(2):
            winds_out[:, 2 * f - 2 + t, :] = state[0, f, t, BASE : BASE + 128].T

    def send_regions(first, last, mine, theirs, send, recv):
        def body(xy, carry):
            px, py = (x + xy % 4) % 4, (y + xy // 4) % 4
            pos = py * 4 + px + (py % 2) * (3 - 2 * px)
            column = (px * 4 + py) * 8
            for j, d in enumerate(ORDER):
                zk = (k + away * 4 + d) % 8
                pz = 2 * zk + z_hi
                to_region = zk * 16 + pos + (zk % 2) * (15 - 2 * pos)
                where = (column + pz % 8, (pz // 8) * 2 + core)
                copy = remote(mine.at[to_region], theirs.at[m], send, recv, where)
                if j == 0:
                    pl.when(xy + away > 0)(copy.start)
                else:
                    copy.start()
            return carry

        if first < last:
            lax.fori_loop(first, last, body, 0)

    def send_winds(first, last):
        send_regions(first, last, winds_out, winds, a2a_send.at[1], a2a_recv.at[1])

    send_regions(0, 16, heights_out, heights, a2a_send.at[0], a2a_recv.at[0])
    send_winds(0, BATCH[0])

    @pl.when(away == 0)
    def _():
        heights[m] = heights_out[region]
        winds[m] = winds_out[region]

    here = (m, slab)

    def wait_all(source, target, send, recv):
        home = remote(source.at[0:127], target.at[0:127], send, recv, here)
        full = remote(source, target, send, recv, here)
        return home, full

    def wait_recv(pair):
        pl.when(away == 0)(pair[0].wait_recv)
        pl.when(away == 1)(pair[1].wait_recv)

    def wait_send(pair):
        pl.when(away == 0)(pair[0].wait_send)
        pl.when(away == 1)(pair[1].wait_send)

    height_wait = wait_all(heights_out, heights, a2a_send.at[0], a2a_recv.at[0])
    wind_wait = wait_all(winds_out, winds, a2a_send.at[1], a2a_recv.at[1])

    @pl.when(jnp.logical_not(obs_home))
    def _():
        obs_copy.wait()

    where_cell = obs_in[0:1]
    picked = lax.broadcasted_iota(jnp.int32, (256, 128), 0).astype(F32) == where_cell
    picked = picked.astype(F32).astype(BF16)
    wait_recv(height_wait)
    field = {}
    for t in range(2):
        field[0, t] = heights[:, t, :]
    flat = jnp.concatenate([field[0, 0], field[0, 1]], axis=1)
    hi = flat.astype(BF16)
    rest = flat - hi.astype(F32)
    mid = rest.astype(BF16)
    low = (rest - mid.astype(F32)).astype(BF16)
    observed = (
        jnp.dot(hi, picked, preferred_element_type=F32)
        + jnp.dot(mid, picked, preferred_element_type=F32)
        + jnp.dot(low, picked, preferred_element_type=F32)
    )
    obs_mean = jnp.mean(observed, axis=0, keepdims=True)
    anomaly = observed - obs_mean
    innovation = obs_in[1:2] - obs_mean
    weight = 10.0 / (1.0 + obs_in[2:3])
    upper = (where_cell >= 128.0).astype(F32)
    by_row = (weight * (1.0 - upper), weight * upper)
    lhs = jnp.concatenate(
        [anomaly * by_row[0], anomaly * by_row[1], jnp.broadcast_to(innovation * by_row[0], (8, 128)),
         jnp.broadcast_to(innovation * by_row[1], (8, 128))], axis=0
    )
    ah, al = halves(anomaly)
    rhs = jnp.concatenate([jnp.concatenate([ah, ah], axis=1), jnp.concatenate([al, al], axis=1)], axis=0)
    sums = lax.dot_general(as_lhs(lhs), rhs, (((1,), (1,)), ((), ())), preferred_element_type=F32)
    sums = sums[:, :128] + sums[:, 128:]
    pulls = jnp.concatenate([sums[256:260], sums[264:268]], axis=0)
    for i in range(4):
        parts[i, 0:32] = sums[32 * i : 32 * i + 32]
        parts[i, 32:64] = sums[128 + 32 * i : 160 + 32 * i]
        parts[i, 64:72] = pulls

    part_copies = []
    for j in range(1, 4):
        other = (ident + j) % 4
        part_copies.append(
            remote(parts.at[other], parts_in.at[j - 1], part_send.at[j - 1], part_recv.at[j - 1], group(other))
        )
        part_copies[-1].start()
    send_winds(BATCH[0], BATCH[1])
    for copy in part_copies:
        copy.wait()
    chunk[...] = (parts[ident] + parts_in[0]) + (parts_in[1] + parts_in[2])

    chunk_copies = []
    for j, o in enumerate(OFFSETS):
        chunk_copies.append(remote(chunk, chunk_in.at[j], chunk_send.at[j], chunk_recv.at[j], neighbour(o)))
        chunk_copies[-1].start()
    send_winds(BATCH[1], BATCH[2])
    for copy in chunk_copies:
        copy.wait()

    pull = []
    for t in range(2):
        total, row = 0.0, 0.0
        for j, o in enumerate((0,) + OFFSETS):
            source = chunk if j == 0 else chunk_in.at[j - 1]
            for q in range(2):
                scale = math.exp(-0.5 * ((-2 * o + q - t) / 2.0) ** 2)
                total = total + scale * source[32 * q : 32 * q + 32]
                row = row + scale * source[64 + 4 * q : 65 + 4 * q]
        grams[ident, 32 * t : 32 * t + 32] = total
        pull.append(row)
    gram_copies = []
    for j in range(1, 4):
        other = (ident + j) % 4
        gram_copies.append(
            remote(grams.at[ident], grams.at[ident], gram_send.at[j - 1], gram_recv.at[j - 1], group(other))
        )
        gram_copies[-1].start()
    send_winds(BATCH[2], 16)
    for copy in gram_copies:
        copy.wait()

    r_id = lax.broadcasted_iota(jnp.int32, (128, 128), 0)
    c_id = lax.broadcasted_iota(jnp.int32, (128, 128), 1)
    eye = (r_id == c_id).astype(F32)
    ys, zs, scales = [], [], []
    for t in range(2):
        g = jnp.concatenate([grams[i, 32 * t : 32 * t + 32] for i in range(4)], axis=0)
        g = g + (127.0 / 1.1) * eye
        trace = jnp.sum(jnp.sum(g * eye, axis=0, keepdims=True), axis=1, keepdims=True)
        scales.append(trace)
        ys.append(g / trace)
        zs.append(None)
    for sweep in range(SWEEPS):
        for t in range(2):
            if sweep == 0:
                correction = 1.5 * eye - 0.5 * ys[t]
                ys[t] = product(as_lhs(ys[t]), as_rhs(correction))
                zs[t] = correction
            else:
                correction = 1.5 * eye - 0.5 * product(as_lhs(zs[t]), as_rhs(ys[t]))
                if sweep < SWEEPS - 1:
                    both = product(
                        jnp.concatenate([as_lhs(ys[t]), as_lhs(zs[t])], axis=0), as_rhs(correction)
                    )
                    ys[t], zs[t] = both[:128], both[128:]
                else:
                    zs[t] = product(as_lhs(zs[t]), as_rhs(correction))

    mixers = []
    for t in range(2):
        z_rhs = as_rhs(zs[t])
        row = jnp.broadcast_to(pull[t], (8, 128))
        row = product(as_lhs(row), z_rhs)
        row = product(as_lhs(row), z_rhs)[0:1] / scales[t]
        mixers.append(as_lhs(zs[t] * (math.sqrt(127.0) * lax.rsqrt(scales[t])) + row))

    wait_recv(wind_wait)
    for f in range(1, 3):
        for t in range(2):
            field[f, t] = winds[:, 2 * f - 2 + t, :]
    for f in range(3):
        for t in range(2):
            mean = jnp.mean(field[f, t], axis=0, keepdims=True)
            back_out[:, 2 * f + t, :] = mean + product(mixers[t], as_rhs(field[f, t] - mean))

    def send_back(xy, carry):
        px, py = (x + xy % 4) % 4, (y + xy // 4) % 4
        column = (px * 4 + py) * 8
        for j, d in enumerate(ORDER):
            pm = column + (zl + away + d) % 8
            copy = remote(back_out.at[pm], back.at[region], a2a_send.at[2], a2a_recv.at[2], (pm, par * 2 + core))
            if j == 0:
                pl.when(xy + away > 0)(copy.start)
            else:
                copy.start()
        return carry

    lax.fori_loop(0, 16, send_back, 0)

    @pl.when(away == 0)
    def _():
        back[region] = back_out[m]

    back_wait = wait_all(back_out, back, a2a_send.at[2], a2a_recv.at[2])
    wait_recv(back_wait)
    for f in range(3):
        for t in range(2):
            out[f, pl.ds(t, 128, stride=2), :] = back[:, 2 * f + t, :]
    wait_send(height_wait)
    wait_send(wind_wait)
    wait_send(back_wait)


def local(prior, cell, value, bins):
    vmem = pl.BlockSpec(memory_space=pltpu.VMEM)
    dma = pltpu.SemaphoreType.DMA
    result = pl.pallas_call(
        kernel,
        out_shape=jax.ShapeDtypeStruct((3, 256, 128), F32),
        in_specs=[pl.BlockSpec(memory_space=pl.ANY), vmem, vmem, vmem],
        out_specs=vmem,
        scratch_shapes=[
            pltpu.VMEM((3, 256, 128), F32),
            pltpu.VMEM((2, 3, 2, ROWS, 128), F32),
            pltpu.VMEM((2, 72, 128), F32),
            pltpu.VMEM((2, 72, 128), F32),
            pltpu.VMEM((8, 128), F32),
            pltpu.VMEM((8, 128), F32),
            pltpu.VMEM((128, 2, 128), F32),
            pltpu.VMEM((128, 4, 128), F32),
            pltpu.VMEM((128, 2, 128), F32),
            pltpu.VMEM((128, 4, 128), F32),
            pltpu.VMEM((4, 72, 128), F32),
            pltpu.VMEM((3, 72, 128), F32),
            pltpu.VMEM((72, 128), F32),
            pltpu.VMEM((4, 72, 128), F32),
            pltpu.VMEM((4, 64, 128), F32),
            pltpu.VMEM((128, 6, 128), F32),
            pltpu.VMEM((128, 6, 128), F32),
            dma, dma((2,)), dma((2,)), dma, dma, dma((3,)), dma((3,)),
            dma((3,)), dma((3,)), dma((4,)), dma((4,)), dma((3,)), dma((3,)),
            pltpu.SemaphoreType.REGULAR,
        ],
        compiler_params=pltpu.CompilerParams(collective_id=0, has_side_effects=True),
    )(prior[0], cell, value, bins)
    return result[None]


def solution(mesh):
    placed = (P("mem", None, None, "slab"), P("mem", "slab"), P("mem", "slab"), P("mem", "slab"))
    return jax.shard_map(
        local, mesh=mesh, in_specs=placed, out_specs=P("mem", None, None, "slab"), check_vma=False
    )
```

```python
import math

import jax
import jax.numpy as jnp
from jax import lax
from jax.experimental import pallas as pl
from jax.experimental.pallas import tpu as pltpu
from jax.sharding import PartitionSpec as P

STEPS = 12
SWEEPS = 8
SIZE = 32
BATCH = (16, 16, 16)
MESH = pl.DeviceIdType.MESH
F32 = jnp.float32
BF16 = jnp.bfloat16

BASE = 24
ROWS = BASE + 128 + BASE
OFFSETS = (1, -1, 2, -2)
ORDER = (0, 7, 1, 6, 2, 5, 3, 4)


def device_of(x, y, z, core):
    return ((x * 4 + y) * 8 + z % 8, (z // 8) * 2 + core)


def region_at(x, y, k):
    pos = y * 4 + x + (y % 2) * (3 - 2 * x)
    pos = pos + (k % 2) * (15 - 2 * pos)
    return k * 16 + pos


def place_of(region):
    k, pos = region // 16, region % 16
    pos = pos + (k % 2) * (15 - 2 * pos)
    y, x = pos // 4, pos % 4
    return x + (y % 2) * (3 - 2 * x), y, k


def halves(a):
    hi = a.astype(BF16)
    return hi, (a - hi.astype(F32)).astype(BF16)


def as_lhs(a):
    return jnp.concatenate(halves(a), axis=1)


def as_rhs(b):
    row = jnp.concatenate(halves(b), axis=1)
    return jnp.concatenate([row, row], axis=0)


def product(lhs, rhs):
    r = jnp.dot(lhs, rhs, preferred_element_type=F32)
    return r[:, :128] + r[:, 128:]


def forecast_block(src, dst, row, size):
    c, n, s = {}, {}, {}
    for f in range(3):
        for t in range(2):
            c[f, t] = src[f, t, row : row + size]
            n[f, t] = src[f, t, row + 1 : row + 1 + size]
            s[f, t] = src[f, t, row - 1 : row - 1 + size]
    for t in range(2):
        if t == 0:
            e = [c[f, 1] for f in range(3)]
            w = [pltpu.roll(c[f, 1], 1, 1) for f in range(3)]
        else:
            e = [pltpu.roll(c[f, 0], 127, 1) for f in range(3)]
            w = [c[f, 0] for f in range(3)]
        h, u, v = (c[f, t] for f in range(3))
        hn, un, vn = (n[f, t] for f in range(3))
        hs, us, vs = (s[f, t] for f in range(3))
        he, ue, ve = e
        hw, uw, vw = w
        flux = (1.0 + he) * ue - (1.0 + hw) * uw + (1.0 + hn) * vn - (1.0 + hs) * vs
        a, b = 0.125 * u, 0.125 * v
        dst[0, t, row : row + size] = 0.6 * h + 0.1 * (he + hw + hn + hs) - 0.125 * flux
        dst[1, t, row : row + size] = (
            0.6 * u + 0.1 * (ue + uw + un + us) - (a * (ue - uw) + b * (un - us)) - 0.125 * (he - hw) + 0.05 * v
        )
        dst[2, t, row : row + size] = (
            0.6 * v + 0.1 * (ve + vw + vn + vs) - (a * (ve - vw) + b * (vn - vs)) - 0.125 * (hn - hs) - 0.05 * u
        )


def kernel(
    prior, cell_hbm, value_hbm, bins_hbm, out,
    cell, value, bins, nat, state, edge, halo_out, halo_in, obs_out, obs_in, heights_out, winds_out, heights, winds,
    parts, parts_in, chunk, chunk_in, grams, back_out, back,
    load_sem, halo_send, halo_recv, obs_send, obs_recv, a2a_send, a2a_recv,
    part_send, part_recv, chunk_send, chunk_recv, gram_send, gram_recv, small_sem, lines,
):
    m, slab = lax.axis_index("mem"), lax.axis_index("slab")
    x, y, zl = m // 32, (m // 8) % 4, m % 8
    z_hi, core = slab // 2, slab % 2
    z = z_hi * 8 + zl
    k, par = z // 2, z % 2
    region = region_at(x, y, k)
    ident = par * 2 + core
    away = (z_hi + par) % 2

    def remote(src, dst, send, recv, where):
        return pltpu.make_async_remote_copy(
            src_ref=src, dst_ref=dst, send_sem=send, recv_sem=recv, device_id=where, device_id_type=MESH
        )

    def group(i):
        return device_of(x, y, 2 * k + i // 2, i % 2)

    def neighbour(o):
        nx, ny, nk = place_of((region + o + 128) % 128)
        return device_of(nx, ny, 2 * nk + par, core)

    load = pltpu.make_async_copy(prior, nat, load_sem)
    load.start()
    small = [
        pltpu.make_async_copy(source, target, small_sem.at[i])
        for i, (source, target) in enumerate(((cell_hbm, cell), (value_hbm, value), (bins_hbm, bins)))
    ]

    barrier = pltpu.get_barrier_semaphore()

    def greet(where):
        pl.semaphore_signal(barrier, inc=1, device_id=where, device_id_type=MESH)

    for side in (1, 3):
        greet((m, (slab + side) % 4))
    for j in range(1, 4):
        greet(group((ident + j) % 4))
    for o in OFFSETS:
        greet(neighbour(o))

    def in_plane(j):
        return ((x + j % 4) % 4 * 4 + (y + j // 4) % 4) * 8 + zl, slab

    def greet_line_and_plane(j, carry):
        pz = (z + j) % 16
        greet((m - zl + pz % 8, (pz // 8) * 2 + core))
        greet(in_plane(j))
        return carry

    def tell_plane(j, carry):
        pl.semaphore_signal(lines, inc=1, device_id=in_plane(j), device_id_type=MESH)
        return carry

    lax.fori_loop(1, 16, greet_line_and_plane, 0)
    for copy in small:
        copy.start()
    load.wait()
    for f in range(3):
        for t in range(2):
            state[0, f, t, BASE : BASE + 128] = nat[f, pl.ds(t, 128, stride=2), :].T
            i = (f * 2 + t) * 12
            halo_out[0, i : i + 12] = state[0, f, t, BASE : BASE + 12]
            halo_out[1, i : i + 12] = state[0, f, t, BASE + 116 : BASE + 128]
    halo = [
        remote(halo_out.at[0], halo_in.at[0], halo_send.at[0], halo_recv.at[0], (m, (slab + 3) % 4)),
        remote(halo_out.at[1], halo_in.at[1], halo_send.at[1], halo_recv.at[1], (m, (slab + 1) % 4)),
    ]

    pl.semaphore_wait(barrier, 39)
    for copy in halo:
        copy.start()
    lax.fori_loop(1, 16, tell_plane, 0)

    def ends_at(target, side, at):
        for f in range(3):
            for t in range(2):
                i = (f * 2 + t) * 12
                target[0, f, t, at : at + 12] = halo_in[side, i : i + 12]

    @pl.when(core == 0)
    def _():
        for f in range(3):
            for t in range(2):
                edge[0, f, t, 24:48] = state[0, f, t, BASE : BASE + 24]
        halo[1].wait_send()
        halo[0].wait_recv()
        ends_at(state, 0, BASE + 128)

    @pl.when(core == 1)
    def _():
        for f in range(3):
            for t in range(2):
                edge[0, f, t, 8:32] = state[0, f, t, BASE + 104 : BASE + 128]
        halo[0].wait_send()
        halo[1].wait_recv()
        ends_at(state, 1, BASE - 12)

    def two_steps(counter, carry):
        for now in range(2):
            for block in range(160 // SIZE):
                forecast_block(state.at[now], state.at[1 - now], BASE - 16 + SIZE * block, SIZE)
        return carry

    lax.fori_loop(0, STEPS // 2, two_steps, 0)

    @pl.when(core == 0)
    def _():
        halo[0].wait_send()
        halo[1].wait_recv()
        ends_at(edge, 1, 12)

    @pl.when(core == 1)
    def _():
        halo[1].wait_send()
        halo[0].wait_recv()
        ends_at(edge, 0, 32)

    def two_edge_steps(counter, carry):
        for now in range(2):
            forecast_block(edge.at[now], edge.at[1 - now], 8, 24)
            forecast_block(edge.at[now], edge.at[1 - now], 32, 16)
        return carry

    lax.fori_loop(0, STEPS // 2, two_edge_steps, 0)

    @pl.when(core == 0)
    def _():
        for f in range(3):
            for t in range(2):
                state[0, f, t, BASE : BASE + 12] = edge[0, f, t, 24:36]

    @pl.when(core == 1)
    def _():
        for f in range(3):
            for t in range(2):
                state[0, f, t, BASE + 116 : BASE + 128] = edge[0, f, t, 20:32]

    pl.semaphore_wait(lines, 15)

    ox, oy, ok = place_of(m)
    for copy in small:
        copy.wait()
    obs_out[0:1] = cell[...].astype(F32)
    obs_out[1:2] = value[...]
    obs_out[2:3] = bins[...].astype(F32)
    obs_where = device_of(ox, oy, 2 * ok + z_hi, core)
    obs_copy = remote(obs_out, obs_in, obs_send, obs_recv, obs_where)
    obs_home = jnp.logical_and(obs_where[0] == m, obs_where[1] == slab)

    @pl.when(jnp.logical_not(obs_home))
    def _():
        obs_copy.start()

    @pl.when(obs_home)
    def _():
        obs_in[...] = obs_out[...]

    for t in range(2):
        heights_out[:, t, :] = state[0, 0, t, BASE : BASE + 128].T
    for f in range(1, 3):
        for t in range(2):
            winds_out[:, 2 * f - 2 + t, :] = state[0, f, t, BASE : BASE + 128].T

    def send_regions(first, last, mine, theirs, send, recv):
        def body(xy, carry):
            px, py = (x + xy % 4) % 4, (y + xy // 4) % 4
            pos = py * 4 + px + (py % 2) * (3 - 2 * px)
            column = (px * 4 + py) * 8
            for j, d in enumerate(ORDER):
                zk = (k + away * 4 + d) % 8
                pz = 2 * zk + z_hi
                to_region = zk * 16 + pos + (zk % 2) * (15 - 2 * pos)
                where = (column + pz % 8, (pz // 8) * 2 + core)
                copy = remote(mine.at[to_region], theirs.at[m], send, recv, where)
                if j == 0:
                    pl.when(xy + away > 0)(copy.start)
                else:
                    copy.start()
            return carry

        if first < last:
            lax.fori_loop(first, last, body, 0)

    def send_winds(first, last):
        send_regions(first, last, winds_out, winds, a2a_send.at[1], a2a_recv.at[1])

    send_regions(0, 16, heights_out, heights, a2a_send.at[0], a2a_recv.at[0])
    send_winds(0, BATCH[0])

    @pl.when(away == 0)
    def _():
        heights[m] = heights_out[region]
        winds[m] = winds_out[region]

    here = (m, slab)

    def wait_all(source, target, send, recv):
        home = remote(source.at[0:127], target.at[0:127], send, recv, here)
        full = remote(source, target, send, recv, here)
        return home, full

    def wait_recv(pair):
        pl.when(away == 0)(pair[0].wait_recv)
        pl.when(away == 1)(pair[1].wait_recv)

    def wait_send(pair):
        pl.when(away == 0)(pair[0].wait_send)
        pl.when(away == 1)(pair[1].wait_send)

    height_wait = wait_all(heights_out, heights, a2a_send.at[0], a2a_recv.at[0])
    wind_wait = wait_all(winds_out, winds, a2a_send.at[1], a2a_recv.at[1])

    @pl.when(jnp.logical_not(obs_home))
    def _():
        obs_copy.wait()

    where_cell = obs_in[0:1]
    picked = lax.broadcasted_iota(jnp.int32, (256, 128), 0).astype(F32) == where_cell
    picked = picked.astype(F32).astype(BF16)
    wait_recv(height_wait)
    field = {}
    for t in range(2):
        field[0, t] = heights[:, t, :]
    flat = jnp.concatenate([field[0, 0], field[0, 1]], axis=1)
    hi = flat.astype(BF16)
    rest = flat - hi.astype(F32)
    mid = rest.astype(BF16)
    low = (rest - mid.astype(F32)).astype(BF16)
    observed = (
        jnp.dot(hi, picked, preferred_element_type=F32)
        + jnp.dot(mid, picked, preferred_element_type=F32)
        + jnp.dot(low, picked, preferred_element_type=F32)
    )
    obs_mean = jnp.mean(observed, axis=0, keepdims=True)
    anomaly = observed - obs_mean
    innovation = obs_in[1:2] - obs_mean
    weight = 10.0 / (1.0 + obs_in[2:3])
    upper = (where_cell >= 128.0).astype(F32)
    by_row = (weight * (1.0 - upper), weight * upper)
    lhs = jnp.concatenate(
        [anomaly * by_row[0], anomaly * by_row[1], jnp.broadcast_to(innovation * by_row[0], (8, 128)),
         jnp.broadcast_to(innovation * by_row[1], (8, 128))], axis=0
    )
    ah, al = halves(anomaly)
    rhs = jnp.concatenate([jnp.concatenate([ah, ah], axis=1), jnp.concatenate([al, al], axis=1)], axis=0)
    sums = lax.dot_general(as_lhs(lhs), rhs, (((1,), (1,)), ((), ())), preferred_element_type=F32)
    sums = sums[:, :128] + sums[:, 128:]
    pulls = jnp.concatenate([sums[256:260], sums[264:268]], axis=0)
    for i in range(4):
        parts[i, 0:32] = sums[32 * i : 32 * i + 32]
        parts[i, 32:64] = sums[128 + 32 * i : 160 + 32 * i]
        parts[i, 64:72] = pulls

    part_copies = []
    for j in range(1, 4):
        other = (ident + j) % 4
        part_copies.append(
            remote(parts.at[other], parts_in.at[j - 1], part_send.at[j - 1], part_recv.at[j - 1], group(other))
        )
        part_copies[-1].start()
    send_winds(BATCH[0], BATCH[1])
    for copy in part_copies:
        copy.wait()
    chunk[...] = (parts[ident] + parts_in[0]) + (parts_in[1] + parts_in[2])

    chunk_copies = []
    for j, o in enumerate(OFFSETS):
        chunk_copies.append(remote(chunk, chunk_in.at[j], chunk_send.at[j], chunk_recv.at[j], neighbour(o)))
        chunk_copies[-1].start()
    send_winds(BATCH[1], BATCH[2])
    for copy in chunk_copies:
        copy.wait()

    pull = []
    for t in range(2):
        total, row = 0.0, 0.0
        for j, o in enumerate((0,) + OFFSETS):
            source = chunk if j == 0 else chunk_in.at[j - 1]
            for q in range(2):
                scale = math.exp(-0.5 * ((-2 * o + q - t) / 2.0) ** 2)
                total = total + scale * source[32 * q : 32 * q + 32]
                row = row + scale * source[64 + 4 * q : 65 + 4 * q]
        grams[ident, 32 * t : 32 * t + 32] = total
        pull.append(row)
    gram_copies = []
    for j in range(1, 4):
        other = (ident + j) % 4
        gram_copies.append(
            remote(grams.at[ident], grams.at[ident], gram_send.at[j - 1], gram_recv.at[j - 1], group(other))
        )
        gram_copies[-1].start()
    send_winds(BATCH[2], 16)
    for copy in gram_copies:
        copy.wait()

    r_id = lax.broadcasted_iota(jnp.int32, (128, 128), 0)
    c_id = lax.broadcasted_iota(jnp.int32, (128, 128), 1)
    eye = (r_id == c_id).astype(F32)
    ys, zs, scales = [], [], []
    for t in range(2):
        g = jnp.concatenate([grams[i, 32 * t : 32 * t + 32] for i in range(4)], axis=0)
        g = g + (127.0 / 1.1) * eye
        trace = jnp.sum(jnp.sum(g * eye, axis=0, keepdims=True), axis=1, keepdims=True)
        scales.append(trace)
        ys.append(g / trace)
        zs.append(None)
    for sweep in range(SWEEPS):
        for t in range(2):
            if sweep == 0:
                correction = 1.5 * eye - 0.5 * ys[t]
                ys[t] = product(as_lhs(ys[t]), as_rhs(correction))
                zs[t] = correction
            else:
                correction = 1.5 * eye - 0.5 * product(as_lhs(zs[t]), as_rhs(ys[t]))
                if sweep < SWEEPS - 1:
                    both = product(
                        jnp.concatenate([as_lhs(ys[t]), as_lhs(zs[t])], axis=0), as_rhs(correction)
                    )
                    ys[t], zs[t] = both[:128], both[128:]
                else:
                    zs[t] = product(as_lhs(zs[t]), as_rhs(correction))

    mixers = []
    for t in range(2):
        z_rhs = as_rhs(zs[t])
        row = jnp.broadcast_to(pull[t], (8, 128))
        row = product(as_lhs(row), z_rhs)
        row = product(as_lhs(row), z_rhs)[0:1] / scales[t]
        mixers.append(as_lhs(zs[t] * (math.sqrt(127.0) * lax.rsqrt(scales[t])) + row))

    wait_recv(wind_wait)
    for f in range(1, 3):
        for t in range(2):
            field[f, t] = winds[:, 2 * f - 2 + t, :]
    for f in range(3):
        for t in range(2):
            mean = jnp.mean(field[f, t], axis=0, keepdims=True)
            back_out[:, 2 * f + t, :] = mean + product(mixers[t], as_rhs(field[f, t] - mean))

    def send_back(xy, carry):
        px, py = (x + xy % 4) % 4, (y + xy // 4) % 4
        column = (px * 4 + py) * 8
        for j, d in enumerate(ORDER):
            pm = column + (zl + away + d) % 8
            copy = remote(back_out.at[pm], back.at[region], a2a_send.at[2], a2a_recv.at[2], (pm, par * 2 + core))
            if j == 0:
                pl.when(xy + away > 0)(copy.start)
            else:
                copy.start()
        return carry

    lax.fori_loop(0, 16, send_back, 0)

    @pl.when(away == 0)
    def _():
        back[region] = back_out[m]

    back_wait = wait_all(back_out, back, a2a_send.at[2], a2a_recv.at[2])
    wait_recv(back_wait)
    for f in range(3):
        for t in range(2):
            out[f, pl.ds(t, 128, stride=2), :] = back[:, 2 * f + t, :]
    wait_send(height_wait)
    wait_send(wind_wait)
    wait_send(back_wait)


def local(prior, cell, value, bins):
    vmem = pl.BlockSpec(memory_space=pltpu.VMEM)
    dma = pltpu.SemaphoreType.DMA
    result = pl.pallas_call(
        kernel,
        out_shape=jax.ShapeDtypeStruct((3, 256, 128), F32),
        in_specs=[pl.BlockSpec(memory_space=pltpu.MemorySpace.HBM)] * 4,
        out_specs=vmem,
        scratch_shapes=[
            pltpu.VMEM((1, 128), jnp.int32),
            pltpu.VMEM((1, 128), F32),
            pltpu.VMEM((1, 128), jnp.int32),
            pltpu.VMEM((3, 256, 128), F32),
            pltpu.VMEM((2, 3, 2, ROWS, 128), F32),
            pltpu.VMEM((2, 3, 2, 56, 128), F32),
            pltpu.VMEM((2, 72, 128), F32),
            pltpu.VMEM((2, 72, 128), F32),
            pltpu.VMEM((8, 128), F32),
            pltpu.VMEM((8, 128), F32),
            pltpu.VMEM((128, 2, 128), F32),
            pltpu.VMEM((128, 4, 128), F32),
            pltpu.VMEM((128, 2, 128), F32),
            pltpu.VMEM((128, 4, 128), F32),
            pltpu.VMEM((4, 72, 128), F32),
            pltpu.VMEM((3, 72, 128), F32),
            pltpu.VMEM((72, 128), F32),
            pltpu.VMEM((4, 72, 128), F32),
            pltpu.VMEM((4, 64, 128), F32),
            pltpu.VMEM((128, 6, 128), F32),
            pltpu.VMEM((128, 6, 128), F32),
            dma, dma((2,)), dma((2,)), dma, dma, dma((3,)), dma((3,)),
            dma((3,)), dma((3,)), dma((4,)), dma((4,)), dma((3,)), dma((3,)),
            dma((3,)), pltpu.SemaphoreType.REGULAR,
        ],
        compiler_params=pltpu.CompilerParams(collective_id=0, has_side_effects=True, vmem_limit_bytes=12 * 2**20),
    )(*(pltpu.with_memory_space_constraint(a, pltpu.MemorySpace.HBM) for a in (prior[0], cell, value, bins)))
    return result[None]


def solution(mesh):
    placed = (P("mem", None, None, "slab"), P("mem", "slab"), P("mem", "slab"), P("mem", "slab"))
    return jax.shard_map(
        local, mesh=mesh, in_specs=placed, out_specs=P("mem", None, None, "slab"), check_vma=False
    )
```

```python
import math

import jax
import jax.numpy as jnp
from jax import lax
from jax.experimental import pallas as pl
from jax.experimental.pallas import tpu as pltpu
from jax.sharding import PartitionSpec as P

STEPS = 12
SWEEPS = 8
SIZE = 32
BATCH = (8, 16, 16)
MESH = pl.DeviceIdType.MESH
F32 = jnp.float32
BF16 = jnp.bfloat16

BASE = 24
ROWS = BASE + 128 + BASE
OFFSETS = (1, -1, 2, -2)
ORDER = (0, 7, 1, 6, 2, 5, 3, 4)


def device_of(x, y, z, core):
    return ((x * 4 + y) * 8 + z % 8, (z // 8) * 2 + core)


def region_at(x, y, k):
    pos = y * 4 + x + (y % 2) * (3 - 2 * x)
    pos = pos + (k % 2) * (15 - 2 * pos)
    return k * 16 + pos


def place_of(region):
    k, pos = region // 16, region % 16
    pos = pos + (k % 2) * (15 - 2 * pos)
    y, x = pos // 4, pos % 4
    return x + (y % 2) * (3 - 2 * x), y, k


def halves(a):
    hi = a.astype(BF16)
    return hi, (a - hi.astype(F32)).astype(BF16)


def as_lhs(a):
    return jnp.concatenate(halves(a), axis=1)


def as_rhs(b):
    row = jnp.concatenate(halves(b), axis=1)
    return jnp.concatenate([row, row], axis=0)


def product(lhs, rhs):
    r = jnp.dot(lhs, rhs, preferred_element_type=F32)
    return r[:, :128] + r[:, 128:]


def forecast_block(src, dst, row, size):
    c, n, s = {}, {}, {}
    for f in range(3):
        for t in range(2):
            c[f, t] = src[f, t, row : row + size]
            n[f, t] = src[f, t, row + 1 : row + 1 + size]
            s[f, t] = src[f, t, row - 1 : row - 1 + size]
    for t in range(2):
        if t == 0:
            e = [c[f, 1] for f in range(3)]
            w = [pltpu.roll(c[f, 1], 1, 1) for f in range(3)]
        else:
            e = [pltpu.roll(c[f, 0], 127, 1) for f in range(3)]
            w = [c[f, 0] for f in range(3)]
        h, u, v = (c[f, t] for f in range(3))
        hn, un, vn = (n[f, t] for f in range(3))
        hs, us, vs = (s[f, t] for f in range(3))
        he, ue, ve = e
        hw, uw, vw = w
        flux = (1.0 + he) * ue - (1.0 + hw) * uw + (1.0 + hn) * vn - (1.0 + hs) * vs
        a, b = 0.125 * u, 0.125 * v
        dst[0, t, row : row + size] = 0.6 * h + 0.1 * (he + hw + hn + hs) - 0.125 * flux
        dst[1, t, row : row + size] = (
            0.6 * u + 0.1 * (ue + uw + un + us) - (a * (ue - uw) + b * (un - us)) - 0.125 * (he - hw) + 0.05 * v
        )
        dst[2, t, row : row + size] = (
            0.6 * v + 0.1 * (ve + vw + vn + vs) - (a * (ve - vw) + b * (vn - vs)) - 0.125 * (hn - hs) - 0.05 * u
        )


def kernel(
    prior, cell_hbm, value_hbm, bins_hbm, out,
    cell, value, bins, nat, state, edge, halo_out, halo_in, obs_out, obs_in, heights_out, winds_out, heights, winds,
    parts, parts_in, chunk, chunk_in, grams, back_out, back,
    load_sem, halo_send, halo_recv, obs_send, obs_recv, a2a_send, a2a_recv,
    part_send, part_recv, chunk_send, chunk_recv, gram_send, gram_recv, small_sem, lines,
):
    m, slab = lax.axis_index("mem"), lax.axis_index("slab")
    x, y, zl = m // 32, (m // 8) % 4, m % 8
    z_hi, core = slab // 2, slab % 2
    z = z_hi * 8 + zl
    k, par = z // 2, z % 2
    region = region_at(x, y, k)
    ident = par * 2 + core
    away = (z_hi + par) % 2

    def remote(src, dst, send, recv, where):
        return pltpu.make_async_remote_copy(
            src_ref=src, dst_ref=dst, send_sem=send, recv_sem=recv, device_id=where, device_id_type=MESH
        )

    def group(i):
        return device_of(x, y, 2 * k + i // 2, i % 2)

    def neighbour(o):
        nx, ny, nk = place_of((region + o + 128) % 128)
        return device_of(nx, ny, 2 * nk + par, core)

    load = pltpu.make_async_copy(prior, nat, load_sem)
    load.start()
    small = [
        pltpu.make_async_copy(source, target, small_sem.at[i])
        for i, (source, target) in enumerate(((cell_hbm, cell), (value_hbm, value), (bins_hbm, bins)))
    ]

    barrier = pltpu.get_barrier_semaphore()

    def greet(where):
        pl.semaphore_signal(barrier, inc=1, device_id=where, device_id_type=MESH)

    for side in (1, 3):
        greet((m, (slab + side) % 4))
    for j in range(1, 4):
        greet(group((ident + j) % 4))
    for o in OFFSETS:
        greet(neighbour(o))

    def in_plane(j):
        return ((x + j % 4) % 4 * 4 + (y + j // 4) % 4) * 8 + zl, slab

    def greet_line_and_plane(j, carry):
        pz = (z + j) % 16
        greet((m - zl + pz % 8, (pz // 8) * 2 + core))
        greet(in_plane(j))
        return carry

    def tell_plane(j, carry):
        pl.semaphore_signal(lines, inc=1, device_id=in_plane(j), device_id_type=MESH)
        return carry

    lax.fori_loop(1, 16, greet_line_and_plane, 0)
    for copy in small:
        copy.start()
    load.wait()
    for f in range(3):
        for t in range(2):
            state[0, f, t, BASE : BASE + 128] = nat[f, pl.ds(t, 128, stride=2), :].T
            i = (f * 2 + t) * 12
            halo_out[0, i : i + 12] = state[0, f, t, BASE : BASE + 12]
            halo_out[1, i : i + 12] = state[0, f, t, BASE + 116 : BASE + 128]
    halo = [
        remote(halo_out.at[0], halo_in.at[0], halo_send.at[0], halo_recv.at[0], (m, (slab + 3) % 4)),
        remote(halo_out.at[1], halo_in.at[1], halo_send.at[1], halo_recv.at[1], (m, (slab + 1) % 4)),
    ]

    pl.semaphore_wait(barrier, 39)
    for copy in halo:
        copy.start()
    lax.fori_loop(1, 16, tell_plane, 0)

    def ends_at(target, side, at):
        for f in range(3):
            for t in range(2):
                i = (f * 2 + t) * 12
                target[0, f, t, at : at + 12] = halo_in[side, i : i + 12]

    @pl.when(core == 0)
    def _():
        for f in range(3):
            for t in range(2):
                edge[0, f, t, 24:48] = state[0, f, t, BASE : BASE + 24]
        halo[1].wait_send()
        halo[0].wait_recv()
        ends_at(state, 0, BASE + 128)

    @pl.when(core == 1)
    def _():
        for f in range(3):
            for t in range(2):
                edge[0, f, t, 8:32] = state[0, f, t, BASE + 104 : BASE + 128]
        halo[0].wait_send()
        halo[1].wait_recv()
        ends_at(state, 1, BASE - 12)

    def two_steps(counter, carry):
        for now in range(2):
            for block in range(160 // SIZE):
                forecast_block(state.at[now], state.at[1 - now], BASE - 16 + SIZE * block, SIZE)
        return carry

    lax.fori_loop(0, STEPS // 2, two_steps, 0)

    @pl.when(core == 0)
    def _():
        halo[0].wait_send()
        halo[1].wait_recv()
        ends_at(edge, 1, 12)

    @pl.when(core == 1)
    def _():
        halo[1].wait_send()
        halo[0].wait_recv()
        ends_at(edge, 0, 32)

    def two_edge_steps(counter, carry):
        for now in range(2):
            forecast_block(edge.at[now], edge.at[1 - now], 8, 24)
            forecast_block(edge.at[now], edge.at[1 - now], 32, 16)
        return carry

    lax.fori_loop(0, STEPS // 2, two_edge_steps, 0)

    @pl.when(core == 0)
    def _():
        for f in range(3):
            for t in range(2):
                state[0, f, t, BASE : BASE + 12] = edge[0, f, t, 24:36]

    @pl.when(core == 1)
    def _():
        for f in range(3):
            for t in range(2):
                state[0, f, t, BASE + 116 : BASE + 128] = edge[0, f, t, 20:32]

    pl.semaphore_wait(lines, 15)

    ox, oy, ok = place_of(m)
    for copy in small:
        copy.wait()
    obs_out[0:1] = cell[...].astype(F32)
    obs_out[1:2] = value[...]
    obs_out[2:3] = bins[...].astype(F32)
    obs_where = device_of(ox, oy, 2 * ok + z_hi, core)
    obs_copy = remote(obs_out, obs_in, obs_send, obs_recv, obs_where)
    obs_home = jnp.logical_and(obs_where[0] == m, obs_where[1] == slab)

    @pl.when(jnp.logical_not(obs_home))
    def _():
        obs_copy.start()

    @pl.when(obs_home)
    def _():
        obs_in[...] = obs_out[...]

    for t in range(2):
        heights_out[:, t, :] = state[0, 0, t, BASE : BASE + 128].T
    for f in range(1, 3):
        for t in range(2):
            winds_out[:, 2 * f - 2 + t, :] = state[0, f, t, BASE : BASE + 128].T

    def send_regions(first, last, mine, theirs, send, recv):
        def body(xy, carry):
            px, py = (x + xy % 4) % 4, (y + xy // 4) % 4
            pos = py * 4 + px + (py % 2) * (3 - 2 * px)
            column = (px * 4 + py) * 8
            for j, d in enumerate(ORDER):
                zk = (k + away * 4 + d) % 8
                pz = 2 * zk + z_hi
                to_region = zk * 16 + pos + (zk % 2) * (15 - 2 * pos)
                where = (column + pz % 8, (pz // 8) * 2 + core)
                copy = remote(mine.at[to_region], theirs.at[m], send, recv, where)
                if j == 0:
                    pl.when(xy + away > 0)(copy.start)
                else:
                    copy.start()
            return carry

        if first < last:
            lax.fori_loop(first, last, body, 0)

    def send_winds(first, last):
        send_regions(first, last, winds_out, winds, a2a_send.at[1], a2a_recv.at[1])

    send_regions(0, 16, heights_out, heights, a2a_send.at[0], a2a_recv.at[0])
    send_winds(0, BATCH[0])

    @pl.when(away == 0)
    def _():
        heights[m] = heights_out[region]
        winds[m] = winds_out[region]

    here = (m, slab)

    def wait_all(source, target, send, recv):
        home = remote(source.at[0:127], target.at[0:127], send, recv, here)
        full = remote(source, target, send, recv, here)
        return home, full

    def wait_recv(pair):
        pl.when(away == 0)(pair[0].wait_recv)
        pl.when(away == 1)(pair[1].wait_recv)

    def wait_send(pair):
        pl.when(away == 0)(pair[0].wait_send)
        pl.when(away == 1)(pair[1].wait_send)

    height_wait = wait_all(heights_out, heights, a2a_send.at[0], a2a_recv.at[0])
    wind_wait = wait_all(winds_out, winds, a2a_send.at[1], a2a_recv.at[1])

    @pl.when(jnp.logical_not(obs_home))
    def _():
        obs_copy.wait()

    where_cell = obs_in[0:1]
    picked = lax.broadcasted_iota(jnp.int32, (256, 128), 0).astype(F32) == where_cell
    picked = picked.astype(F32).astype(BF16)
    wait_recv(height_wait)
    field = {}
    for t in range(2):
        field[0, t] = heights[:, t, :]
    flat = jnp.concatenate([field[0, 0], field[0, 1]], axis=1)
    hi = flat.astype(BF16)
    rest = flat - hi.astype(F32)
    mid = rest.astype(BF16)
    low = (rest - mid.astype(F32)).astype(BF16)
    observed = (
        jnp.dot(hi, picked, preferred_element_type=F32)
        + jnp.dot(mid, picked, preferred_element_type=F32)
        + jnp.dot(low, picked, preferred_element_type=F32)
    )
    obs_mean = jnp.mean(observed, axis=0, keepdims=True)
    anomaly = observed - obs_mean
    innovation = obs_in[1:2] - obs_mean
    weight = 10.0 / (1.0 + obs_in[2:3])
    upper = (where_cell >= 128.0).astype(F32)
    by_row = (weight * (1.0 - upper), weight * upper)
    lhs = jnp.concatenate(
        [anomaly * by_row[0], anomaly * by_row[1], jnp.broadcast_to(innovation * by_row[0], (8, 128)),
         jnp.broadcast_to(innovation * by_row[1], (8, 128))], axis=0
    )
    ah, al = halves(anomaly)
    rhs = jnp.concatenate([jnp.concatenate([ah, ah], axis=1), jnp.concatenate([al, al], axis=1)], axis=0)
    sums = lax.dot_general(as_lhs(lhs), rhs, (((1,), (1,)), ((), ())), preferred_element_type=F32)
    sums = sums[:, :128] + sums[:, 128:]
    pulls = jnp.concatenate([sums[256:260], sums[264:268]], axis=0)
    for i in range(4):
        parts[i, 0:32] = sums[32 * i : 32 * i + 32]
        parts[i, 32:64] = sums[128 + 32 * i : 160 + 32 * i]
        parts[i, 64:72] = pulls

    part_copies = []
    for j in range(1, 4):
        other = (ident + j) % 4
        part_copies.append(
            remote(parts.at[other], parts_in.at[j - 1], part_send.at[j - 1], part_recv.at[j - 1], group(other))
        )
        part_copies[-1].start()
    send_winds(BATCH[0], BATCH[1])
    for copy in part_copies:
        copy.wait()
    chunk[...] = (parts[ident] + parts_in[0]) + (parts_in[1] + parts_in[2])

    chunk_copies = []
    for j, o in enumerate(OFFSETS):
        chunk_copies.append(remote(chunk, chunk_in.at[j], chunk_send.at[j], chunk_recv.at[j], neighbour(o)))
        chunk_copies[-1].start()
    send_winds(BATCH[1], BATCH[2])
    for copy in chunk_copies:
        copy.wait()

    pull = []
    for t in range(2):
        total, row = 0.0, 0.0
        for j, o in enumerate((0,) + OFFSETS):
            source = chunk if j == 0 else chunk_in.at[j - 1]
            for q in range(2):
                scale = math.exp(-0.5 * ((-2 * o + q - t) / 2.0) ** 2)
                total = total + scale * source[32 * q : 32 * q + 32]
                row = row + scale * source[64 + 4 * q : 65 + 4 * q]
        grams[ident, 32 * t : 32 * t + 32] = total
        pull.append(row)
    gram_copies = []
    for j in range(1, 4):
        other = (ident + j) % 4
        gram_copies.append(
            remote(grams.at[ident], grams.at[ident], gram_send.at[j - 1], gram_recv.at[j - 1], group(other))
        )
        gram_copies[-1].start()
    send_winds(BATCH[2], 16)
    for copy in gram_copies:
        copy.wait()

    r_id = lax.broadcasted_iota(jnp.int32, (128, 128), 0)
    c_id = lax.broadcasted_iota(jnp.int32, (128, 128), 1)
    eye = (r_id == c_id).astype(F32)
    ys, zs, scales = [], [], []
    for t in range(2):
        g = jnp.concatenate([grams[i, 32 * t : 32 * t + 32] for i in range(4)], axis=0)
        g = g + (127.0 / 1.1) * eye
        trace = jnp.sum(jnp.sum(g * eye, axis=0, keepdims=True), axis=1, keepdims=True)
        scales.append(trace)
        ys.append(g / trace)
        zs.append(None)
    for sweep in range(SWEEPS):
        for t in range(2):
            if sweep == 0:
                correction = 1.5 * eye - 0.5 * ys[t]
                ys[t] = product(as_lhs(ys[t]), as_rhs(correction))
                zs[t] = correction
            else:
                correction = 1.5 * eye - 0.5 * product(as_lhs(zs[t]), as_rhs(ys[t]))
                if sweep < SWEEPS - 1:
                    both = product(
                        jnp.concatenate([as_lhs(ys[t]), as_lhs(zs[t])], axis=0), as_rhs(correction)
                    )
                    ys[t], zs[t] = both[:128], both[128:]
                else:
                    zs[t] = product(as_lhs(zs[t]), as_rhs(correction))

    mixers = []
    for t in range(2):
        z_rhs = as_rhs(zs[t])
        row = jnp.broadcast_to(pull[t], (8, 128))
        row = product(as_lhs(row), z_rhs)
        row = product(as_lhs(row), z_rhs)[0:1] / scales[t]
        mixers.append(as_lhs(zs[t] * (math.sqrt(127.0) * lax.rsqrt(scales[t])) + row))

    wait_recv(wind_wait)
    for f in range(1, 3):
        for t in range(2):
            field[f, t] = winds[:, 2 * f - 2 + t, :]
    for f in range(3):
        for t in range(2):
            mean = jnp.mean(field[f, t], axis=0, keepdims=True)
            back_out[:, 2 * f + t, :] = mean + product(mixers[t], as_rhs(field[f, t] - mean))

    def send_back(xy, carry):
        px, py = (x + xy % 4) % 4, (y + xy // 4) % 4
        column = (px * 4 + py) * 8
        for j, d in enumerate(ORDER):
            pm = column + (zl + away + d) % 8
            copy = remote(back_out.at[pm], back.at[region], a2a_send.at[2], a2a_recv.at[2], (pm, par * 2 + core))
            if j == 0:
                pl.when(xy + away > 0)(copy.start)
            else:
                copy.start()
        return carry

    lax.fori_loop(0, 16, send_back, 0)

    @pl.when(away == 0)
    def _():
        back[region] = back_out[m]

    back_wait = wait_all(back_out, back, a2a_send.at[2], a2a_recv.at[2])
    wait_recv(back_wait)
    for f in range(3):
        for t in range(2):
            out[f, pl.ds(t, 128, stride=2), :] = back[:, 2 * f + t, :]
    wait_send(height_wait)
    wait_send(wind_wait)
    wait_send(back_wait)


def local(prior, cell, value, bins):
    vmem = pl.BlockSpec(memory_space=pltpu.VMEM)
    dma = pltpu.SemaphoreType.DMA
    result = pl.pallas_call(
        kernel,
        out_shape=jax.ShapeDtypeStruct((3, 256, 128), F32),
        in_specs=[pl.BlockSpec(memory_space=pltpu.MemorySpace.HBM)] * 4,
        out_specs=vmem,
        scratch_shapes=[
            pltpu.VMEM((1, 128), jnp.int32),
            pltpu.VMEM((1, 128), F32),
            pltpu.VMEM((1, 128), jnp.int32),
            pltpu.VMEM((3, 256, 128), F32),
            pltpu.VMEM((2, 3, 2, ROWS, 128), F32),
            pltpu.VMEM((2, 3, 2, 56, 128), F32),
            pltpu.VMEM((2, 72, 128), F32),
            pltpu.VMEM((2, 72, 128), F32),
            pltpu.VMEM((8, 128), F32),
            pltpu.VMEM((8, 128), F32),
            pltpu.VMEM((128, 2, 128), F32),
            pltpu.VMEM((128, 4, 128), F32),
            pltpu.VMEM((128, 2, 128), F32),
            pltpu.VMEM((128, 4, 128), F32),
            pltpu.VMEM((4, 72, 128), F32),
            pltpu.VMEM((3, 72, 128), F32),
            pltpu.VMEM((72, 128), F32),
            pltpu.VMEM((4, 72, 128), F32),
            pltpu.VMEM((4, 64, 128), F32),
            pltpu.VMEM((128, 6, 128), F32),
            pltpu.VMEM((128, 6, 128), F32),
            dma, dma((2,)), dma((2,)), dma, dma, dma((3,)), dma((3,)),
            dma((3,)), dma((3,)), dma((4,)), dma((4,)), dma((3,)), dma((3,)),
            dma((3,)), pltpu.SemaphoreType.REGULAR,
        ],
        compiler_params=pltpu.CompilerParams(collective_id=0, has_side_effects=True, vmem_limit_bytes=12 * 2**20),
    )(*(pltpu.with_memory_space_constraint(a, pltpu.MemorySpace.HBM) for a in (prior[0], cell, value, bins)))
    return result[None]


def solution(mesh):
    placed = (P("mem", None, None, "slab"), P("mem", "slab"), P("mem", "slab"), P("mem", "slab"))
    return jax.shard_map(
        local, mesh=mesh, in_specs=placed, out_specs=P("mem", None, None, "slab"), check_vma=False
    )
```
